32 devices in a mesh: dp: 8 (over z, y), tensor: 4 (over x, core).
Axes of the slice: x: 2, y: 2, z: 4, core: 2. Of those that a mesh axis runs over, the one named last changes fastest.
Arguments:
- patches: bfloat16 [8192, 1280], P('dp'), may hold values from -27 to 27
- norm_gain: float32 [1280], replicated, may hold values from 0.1 to 1.9
- norm_bias: float32 [1280], replicated, may hold values from -3 to 3
- first_weight: bfloat16 [5120, 5120], P(None, 'tensor'), may hold values from -0.078125 to 0.078125
- first_bias: float32 [5120], P('tensor'), may hold values from -3 to 3
- second_weight: bfloat16 [5120, 8192], P('tensor', 'dp'), may hold values from -0.078125 to 0.078125
- second_bias: float32 [8192], P('tensor'), may hold values from -2 to 2
- text_embeds: bfloat16 [4096, 8192], P('dp', 'tensor'), may hold values from -36 to 36
- final_gain: float32 [8192], P('tensor'), may hold values from 0.1 to 1.9
- image_grids: int32 [8, 4, 2], replicated, may hold values from 2 to 8, as said below
- routing: int32 [8, 4], replicated, may hold values from 0 to 3, each once within a row
Outputs:
- embeddings: bfloat16 [4096, 8192], P('dp', 'tensor')
- normed: bfloat16 [4096, 8192], P('dp', 'tensor')
The draws below stay inside these ranges and needn't reach their ends.
Inputs may be any that keep to these rules, and one draw needn't show every extreme that they name: `image_grids`: each image is a grid of 3 to 8 rows by 2 to 8 columns of merged tokens; in every draw some image is 8 by 8. `routing`: each row names every offset 0 to 3 once.
All inputs are finite; a program needn't handle non-finite values.
Results may differ from the reference program's by a relative error of at most 0.006.
Values may be sent and summed in bfloat16 or wider, within the bound.
A program may use at most 128 MiB of HBM per device.

```python
import jax
import jax.numpy as jnp
from jax import lax

D_VIT = 1280
D = 8192
D_MERGE = 5120
BLOCKS = 4
SLOTS = 256
CAP = 64
SEQ = 512
SHARDS = 8
PATCHES = 8192
TOTAL_SEQ = 4096
N_TENSOR = 4


def draw_patches(key, part):
    keys = jax.random.split(jax.random.fold_in(key, 11), 3)
    row_scale = jnp.exp(jax.random.uniform(keys[1], (PATCHES, 1), jnp.float32, jnp.log(0.5), jnp.log(5.0)))
    row_offset = jax.random.uniform(keys[2], (PATCHES, 1), jnp.float32, -1.0, 1.0)
    base = jax.random.normal(keys[0], (PATCHES, D_VIT), jnp.float32)
    base = jnp.clip(base, -5.0, 5.0)
    return (base * row_scale + row_offset).astype(jnp.bfloat16)


def draw_text_embeds(key, part):
    keys = jax.random.split(jax.random.fold_in(key, 23), 3)
    column_ids = jnp.arange(D, dtype=jnp.float32)
    column_scale = 0.6 * jnp.power(3.0, column_ids / (D - 1)) * jax.random.uniform(keys[1], (D,), jnp.float32, 0.7, 1.3)
    row_scale = jnp.exp(jax.random.uniform(keys[2], (TOTAL_SEQ, 1), jnp.float32, jnp.log(0.3), jnp.log(3.0)))
    base = jax.random.normal(keys[0], (TOTAL_SEQ, D), jnp.float32)
    base = jnp.clip(base, -5.0, 5.0)
    return (base * row_scale * column_scale[None, :]).astype(jnp.bfloat16)


def draw_image_grids(key, part):
    keys = jax.random.split(jax.random.fold_in(key, 37), 4)
    grid_rows = jax.random.randint(keys[0], (SHARDS, BLOCKS), 3, 9)
    grid_columns = jax.random.randint(keys[1], (SHARDS, BLOCKS), 2, CAP // 8 + 1)
    full_shard = jax.random.randint(keys[2], (), 0, SHARDS)
    full_block = jax.random.randint(keys[3], (), 0, BLOCKS)
    shard_ids = jnp.arange(SHARDS, dtype=jnp.int32)[:, None]
    block_ids = jnp.arange(BLOCKS, dtype=jnp.int32)[None, :]
    target = (shard_ids == full_shard) & (block_ids == full_block)
    grid_rows = jnp.where(target, 8, grid_rows)
    grid_columns = jnp.where(target, CAP // 8, grid_columns)
    return jnp.stack([grid_rows, grid_columns], axis=-1).astype(jnp.int32)


def levels(own_key, shape, pieces, smallest, largest):
    def one(dim, shards_of):
        steps = jax.random.uniform(jax.random.fold_in(jax.random.fold_in(own_key, 6), dim), (shards_of,), jnp.float32, smallest / len(pieces), largest / len(pieces))
        return jnp.repeat(jnp.exp(steps), shape[dim] // shards_of).reshape((-1,) + (1,) * (len(shape) - dim - 1))

    loudness = one(*pieces[0])
    for cut in pieces[1:]:
        loudness = loudness * one(*cut)
    return loudness


def normal_values(own_key, shape, width, most, cuts=(), kind=jnp.bfloat16):
    level = levels(own_key, shape, cuts, -0.22, 0.18) if cuts else 1.0
    drawn = jax.random.normal(own_key, shape, jnp.float32) * width * level
    return jnp.minimum(jnp.maximum(drawn, -most), most).astype(kind)


def setup_inputs(seed: int = 0) -> dict:
    seeds = jax.random.split(jax.random.key(seed), 12)
    patches = draw_patches(jax.random.fold_in(seeds[11], 71), 0)
    norm_gain = jnp.clip(1.0 + 0.18 * jax.random.normal(seeds[1], (D_VIT,), jnp.float32), 0.1, 1.9)
    norm_bias = normal_values(seeds[2], (D_VIT,), 0.5, 3.0, (), jnp.float32)
    first_weight = normal_values(seeds[3], (D_MERGE, D_MERGE), D_MERGE ** -0.5, 0.078125, ((1, 4),))
    first_bias = normal_values(seeds[4], (D_MERGE,), 0.5, 3.0, ((0, 4),), jnp.float32)
    second_weight = normal_values(seeds[5], (D_MERGE, D), D_MERGE ** -0.5, 0.078125, ((0, 4), (1, 8)))
    second_bias = normal_values(seeds[6], (D,), 0.3, 2.0, ((0, 4),), jnp.float32)
    text_embeds = draw_text_embeds(jax.random.fold_in(seeds[11], 71), 0)
    final_gain = jnp.clip(1.0 + 0.18 * jax.random.normal(seeds[8], (D,), jnp.float32), 0.1, 1.9)
    image_grids = draw_image_grids(jax.random.fold_in(seeds[11], 71), 0)
    routing = jax.vmap(lambda own: jax.random.permutation(own, BLOCKS))(jax.random.split(seeds[10], SHARDS)).reshape((SHARDS, BLOCKS)).astype(jnp.int32)
    return {"patches": patches, "norm_gain": norm_gain, "norm_bias": norm_bias, "first_weight": first_weight, "first_bias": first_bias, "second_weight": second_weight, "second_bias": second_bias, "text_embeds": text_embeds, "final_gain": final_gain, "image_grids": image_grids, "routing": routing}


def reference(patches, norm_gain, norm_bias, first_weight, first_bias, second_weight, second_bias, text_embeds, final_gain, image_grids, routing):
    patch_values = patches.astype(jnp.float32)
    centered = patch_values - lax.optimization_barrier(jnp.mean(patch_values, axis=-1, keepdims=True))
    variance = lax.optimization_barrier(jnp.mean(centered * centered, axis=-1, keepdims=True))
    normed_patches = centered * lax.rsqrt(variance + 1e-06) * norm_gain + norm_bias
    merged = normed_patches.reshape(-1, D_MERGE).astype(jnp.bfloat16)
    hidden = jax.nn.gelu(jnp.dot(merged, first_weight, preferred_element_type=jnp.float32) + first_bias, approximate=False).astype(jnp.bfloat16)
    group_width = D_MERGE // N_TENSOR
    summed = jnp.zeros((hidden.shape[0], D), jnp.float32)
    for group in range(N_TENSOR):
        partial_value = jnp.dot(hidden[:, group * group_width:(group + 1) * group_width], second_weight[group * group_width:(group + 1) * group_width], preferred_element_type=jnp.float32).astype(jnp.bfloat16)
        partial_value = lax.optimization_barrier(partial_value)
        summed = summed + partial_value.astype(jnp.float32)
    projected = (summed + second_bias).astype(jnp.bfloat16)
    counts_all = (image_grids[:, :, 0] * image_grids[:, :, 1]).astype(jnp.int32)
    shard_ids = jnp.arange(SHARDS, dtype=jnp.int32)[:, None]
    stride_ids = jnp.arange(BLOCKS, dtype=jnp.int32)[None, :]
    source_shard = ((shard_ids - stride_ids) % SHARDS).astype(jnp.int32)
    source_routing = routing[source_shard]
    block_ids = jnp.arange(BLOCKS, dtype=jnp.int32)[None, None, :]
    chosen = lax.optimization_barrier(jnp.sum(jnp.where(source_routing == stride_ids[:, :, None], block_ids, 0), axis=-1)).astype(jnp.int32)
    lengths = counts_all[source_shard, chosen]
    starts = (jnp.cumsum(lengths, axis=1) - lengths).astype(jnp.int32)
    totals = lax.optimization_barrier(jnp.sum(lengths, axis=1))
    position = jnp.arange(SEQ, dtype=jnp.int32)[None, :]
    which = lax.optimization_barrier(jnp.sum((position[:, :, None] >= starts[:, None, 1:]).astype(jnp.int32), axis=-1)).astype(jnp.int32)
    start_at = jnp.take_along_axis(starts, which, axis=1)
    source_at = jnp.take_along_axis(source_shard, which, axis=1)
    chosen_at = jnp.take_along_axis(chosen, which, axis=1)
    valid = position < totals[:, None]
    row_index = jnp.where(valid, source_at * SLOTS + chosen_at * CAP + position - start_at, 0).astype(jnp.int32)
    image_rows = jnp.take(projected, row_index.reshape(-1), axis=0).reshape(SHARDS, SEQ, D)
    text_rows = text_embeds.reshape(SHARDS, SEQ, D)
    embeddings = jnp.where(valid[:, :, None], image_rows, text_rows).reshape(SHARDS * SEQ, D)
    embed_values = embeddings.astype(jnp.float32)
    mean_square = lax.optimization_barrier(jnp.mean(embed_values * embed_values, axis=-1, keepdims=True))
    normed = (embed_values * lax.rsqrt(mean_square + 1e-06) * final_gain).astype(jnp.bfloat16)
    return (embeddings, normed)
```

```python
import jax
import jax.numpy as jnp
from jax import lax
from jax.sharding import PartitionSpec as P


def per_device(
    patches,
    norm_gain,
    norm_bias,
    first_weight,
    first_bias,
    second_weight,
    second_bias,
    text_embeds,
    final_gain,
    image_grids,
    routing,
):
    own_index = lax.axis_index("dp")
    own_group = lax.axis_index("tensor")
    shard_count = lax.axis_size("dp")
    group_count = lax.axis_size("tensor")
    block_total = image_grids.shape[1]
    slot_rows = patches.shape[0] * patches.shape[1] // first_weight.shape[0]
    cap_rows = slot_rows // block_total
    seq_rows, feature_width = text_embeds.shape
    slot_ids = jnp.arange(block_total, dtype=jnp.int32)

    chosen = jnp.argmax(routing[:, None, :] == slot_ids[None, :, None], axis=-1)
    counts = jnp.take_along_axis(image_grids[:, :, 0] * image_grids[:, :, 1], chosen, axis=1)

    patch_values = patches.astype(jnp.float32)
    centered = patch_values - jnp.mean(patch_values, axis=-1, keepdims=True)
    variance = jnp.mean(centered * centered, axis=-1, keepdims=True)
    normed_patches = centered * lax.rsqrt(variance + 1e-06) * norm_gain + norm_bias
    merged = normed_patches.reshape(-1, first_weight.shape[0]).astype(jnp.bfloat16)
    hidden = jax.nn.gelu(
        jnp.dot(merged, first_weight, preferred_element_type=jnp.float32) + first_bias,
        approximate=False,
    ).astype(jnp.bfloat16)
    own_chosen = lax.dynamic_index_in_dim(chosen, own_index, 0, keepdims=False)
    hidden_blocks = hidden.reshape(block_total, cap_rows, -1)
    hidden = jnp.concatenate(
        [lax.dynamic_index_in_dim(hidden_blocks, own_chosen[k], 0, keepdims=False) for k in range(block_total)], axis=0
    )
    partial_value = jnp.dot(
        lax.all_gather(hidden, "dp", axis=0, tiled=True),
        second_weight,
        preferred_element_type=jnp.float32,
    ).astype(jnp.bfloat16)
    by_stride = partial_value.reshape(shard_count, block_total, cap_rows, -1)
    pieces = by_stride.reshape(shard_count, group_count, -1, by_stride.shape[-1])
    summed = lax.psum_scatter(pieces, "tensor", scatter_dimension=1, tiled=True)
    summed = summed.reshape(shard_count, -1, pieces.shape[-1])
    own_stride = own_group * block_total // group_count
    twice = jnp.concatenate([summed, summed], axis=0)
    rolled = lax.dynamic_slice_in_dim(twice, (shard_count - own_stride) % shard_count, shard_count, 0)
    wide = lax.all_to_all(rolled, "dp", split_axis=0, concat_axis=2, tiled=True)
    wide = wide.reshape(wide.shape[1], -1)
    block_rows = lax.all_to_all(wide, "tensor", split_axis=1, concat_axis=0, tiled=True)
    block_rows = (block_rows.astype(jnp.float32) + second_bias).astype(jnp.bfloat16)
    block_rows = block_rows.reshape(block_total, cap_rows, feature_width)

    image_rows = jnp.zeros((seq_rows, feature_width), jnp.bfloat16)
    filled_rows = jnp.zeros((), jnp.int32)
    zero_index = jnp.zeros((), jnp.int32)
    for stride in range(block_total):
        source_counts = lax.dynamic_index_in_dim(counts, (own_index - stride) % shard_count, 0, keepdims=False)
        image_rows = lax.dynamic_update_slice(image_rows, block_rows[stride], (filled_rows, zero_index))
        filled_rows = filled_rows + source_counts[stride]
    position = jnp.arange(seq_rows, dtype=jnp.int32)[:, None]
    embeddings = jnp.where(position < filled_rows, image_rows, text_embeds)
    embed_values = embeddings.astype(jnp.float32)
    square_total = lax.psum(jnp.sum(embed_values * embed_values, axis=-1), "tensor")
    scale_rows = lax.rsqrt(square_total / (feature_width * group_count) + 1e-06)
    normed = (embed_values * scale_rows[:, None] * final_gain).astype(jnp.bfloat16)
    return (embeddings, normed)


def solution(mesh):
    placed = (
        P("dp", None),
        P(),
        P(),
        P(None, "tensor"),
        P("tensor"),
        P("tensor", "dp"),
        P("tensor"),
        P("dp", "tensor"),
        P("tensor"),
        P(),
        P(),
    )
    return jax.shard_map(
        per_device,
        mesh=mesh,
        in_specs=placed,
        out_specs=(P("dp", "tensor"), P("dp", "tensor")),
        check_vma=False,
    )
```

```python
import functools

import jax
import jax.numpy as jnp
from jax import lax
from jax.experimental import pallas as pl
from jax.experimental.pallas import tpu as pltpu
from jax.sharding import PartitionSpec as P

VMEM_LIMIT = 56 * 1024 * 1024


def hidden_kernel(per_token, patches_ref, gain_ref, bias_ref, weight_ref, first_bias_ref, index_ref, out_ref, rows_ref, total_ref):
    step = pl.program_id(0)
    tokens = out_ref.shape[0]

    @pl.when(step == 0)
    def _():
        gain = gain_ref[...]
        bias = bias_ref[...]

        def chunk(i, carry):
            span = pl.ds(pl.multiple_of(i * 128, 128), 128)
            values = patches_ref[span, :].astype(jnp.float32)
            centered = values - jnp.mean(values, axis=-1, keepdims=True)
            variance = jnp.mean(centered * centered, axis=-1, keepdims=True)
            normed = centered * lax.rsqrt(variance + 1e-06) * gain + bias
            for c in range(normed.shape[1] // 128):
                rows_ref[c, span, :] = normed[:, c * 128:(c + 1) * 128]
            return carry

        lax.fori_loop(0, patches_ref.shape[0] // 128, chunk, 0)
        total_ref[...] = jnp.zeros_like(total_ref)

    strips = [rows_ref[c, pl.ds(step, tokens, stride=per_token), :] for c in range(rows_ref.shape[0])]
    merged = jnp.concatenate(strips, axis=1).astype(jnp.bfloat16)
    total_ref[...] += jnp.dot(merged, weight_ref[...], preferred_element_type=jnp.float32)

    @pl.when(step == per_token - 1)
    def _():
        x = total_ref[...] + first_bias_ref[...]
        hidden = (0.5 * x * (1.0 + lax.erf(x * (0.5 ** 0.5)))).astype(jnp.bfloat16)
        columns = lax.broadcasted_iota(jnp.int32, (tokens, tokens), 1)
        pick = (columns == index_ref[...]).astype(jnp.bfloat16)
        out_ref[...] = jnp.dot(pick, hidden, preferred_element_type=jnp.float32).astype(jnp.bfloat16)


def compact_hidden(patches, norm_gain, norm_bias, first_weight, first_bias, index):
    width = patches.shape[1]
    per_token = first_weight.shape[0] // width
    tokens = patches.shape[0] // per_token
    out_width = first_weight.shape[1]
    whole = lambda shape: pl.BlockSpec(shape, lambda j: (0,) * len(shape))
    return pl.pallas_call(
        functools.partial(hidden_kernel, per_token),
        grid=(per_token,),
        in_specs=[
            whole(patches.shape),
            whole((1, width)),
            whole((1, width)),
            pl.BlockSpec((width, out_width), lambda j: (j, 0)),
            whole((1, out_width)),
            whole((tokens, 1)),
        ],
        out_specs=whole((tokens, out_width)),
        out_shape=jax.ShapeDtypeStruct((tokens, out_width), jnp.bfloat16),
        scratch_shapes=[
            pltpu.VMEM((width // 128, patches.shape[0], 128), jnp.float32),
            pltpu.VMEM((tokens, out_width), jnp.float32),
        ],
        compiler_params=pltpu.CompilerParams(vmem_limit_bytes=VMEM_LIMIT),
        cost_estimate=pl.CostEstimate(
            flops=2 * tokens * first_weight.size, bytes_accessed=2 * first_weight.size, transcendentals=0
        ),
        name="compact_hidden",
    )(patches, norm_gain[None], norm_bias[None], first_weight, first_bias[None], index[:, None])


def project_kernel(strides, *refs):
    index_ref, weight_ref, out_ref = refs[strides], refs[strides + 1], refs[strides + 2]
    rows = out_ref.shape[1]
    index = index_ref[0]
    columns = lax.broadcasted_iota(jnp.int32, (rows, rows), 1)
    total = None
    for k in range(strides):
        pick = (columns + k * rows == index).astype(jnp.bfloat16)
        term = jnp.dot(pick, refs[k][0], preferred_element_type=jnp.float32)
        total = term if total is None else total + term
    out_ref[0] = jnp.dot(total.astype(jnp.bfloat16), weight_ref[...], preferred_element_type=jnp.float32).astype(jnp.bfloat16)


def project(gathered, second_weight, index, strides):
    shards, rows, depth = gathered.shape
    width = second_weight.shape[1]
    source = lambda k: pl.BlockSpec((1, rows, depth), lambda e: ((e + shards - k) % shards, 0, 0))
    return pl.pallas_call(
        functools.partial(project_kernel, strides),
        grid=(shards,),
        in_specs=[source(k) for k in range(strides)]
        + [pl.BlockSpec((1, rows, 1), lambda e: (e, 0, 0)), pl.BlockSpec((depth, width), lambda e: (0, 0))],
        out_specs=pl.BlockSpec((1, rows, width), lambda e: (e, 0, 0)),
        out_shape=jax.ShapeDtypeStruct((shards, rows, width), jnp.bfloat16),
        compiler_params=pltpu.CompilerParams(vmem_limit_bytes=VMEM_LIMIT),
        cost_estimate=pl.CostEstimate(
            flops=2 * shards * rows * depth * width, bytes_accessed=4 * gathered.size, transcendentals=0
        ),
        name="project",
    )(*([gathered] * strides), index[:, :, None], second_weight)


def per_device(
    patches,
    norm_gain,
    norm_bias,
    first_weight,
    first_bias,
    second_weight,
    second_bias,
    text_embeds,
    final_gain,
    image_grids,
    routing,
):
    own_index = lax.axis_index("dp")
    shards = lax.axis_size("dp")
    groups = lax.axis_size("tensor")
    strides = image_grids.shape[1]
    slots = patches.shape[0] * patches.shape[1] // first_weight.shape[0]
    cap = slots // strides
    seq_rows, feature_width = text_embeds.shape
    slot_ids = jnp.arange(strides, dtype=jnp.int32)
    lower = (slot_ids[:, None] < slot_ids[None, :]).astype(jnp.int32)

    is_at = (routing[:, None, :] == slot_ids[None, :, None]).astype(jnp.int32)
    areas = image_grids[:, :, 0] * image_grids[:, :, 1]
    counts = jnp.sum(is_at * areas[:, None, :], axis=-1)
    chosen = jnp.sum(is_at * slot_ids, axis=-1)
    starts = jnp.sum(counts[:, :, None] * lower, axis=1)
    arriving = jnp.stack([jnp.roll(counts[:, k], k) for k in range(strides)], axis=1)
    source_starts = jnp.stack([jnp.roll(starts[:, k], k) for k in range(strides)], axis=1)
    laid_at = jnp.sum(arriving[:, :, None] * lower, axis=1)
    filled = jnp.sum(arriving, axis=1)
    most = jnp.maximum(jnp.max(jnp.sum(counts, axis=1)), jnp.max(filled))

    position = jnp.arange(slots, dtype=jnp.int32)
    own = lambda table: lax.dynamic_index_in_dim(table, own_index, 0, keepdims=False)
    inside = position[:, None] - own(starts)[None, :]
    live = (inside >= 0) & (inside < own(counts)[None, :])
    own_pick = jnp.sum(jnp.where(live, own(chosen)[None, :] * cap + inside + 1, 0), axis=1) - 1
    hidden = compact_hidden(patches, norm_gain, norm_bias, first_weight, first_bias, own_pick)

    def image_part(rows):
        inside = position[None, :rows, None] - laid_at[:, None, :]
        live = (inside >= 0) & (inside < arriving[:, None, :])
        index = jnp.sum(
            jnp.where(live, slot_ids * rows + source_starts[:, None, :] + inside + 1, 0), axis=2
        ) - 1
        gathered = lax.all_gather(hidden[:rows], "dp", axis=0)
        partial_value = project(gathered, second_weight, index, strides)
        pieces = partial_value.reshape(shards, groups, rows // groups, -1)
        summed = lax.psum_scatter(pieces, "tensor", scatter_dimension=1, tiled=True)
        summed = summed.reshape(shards, rows // groups, -1)
        wide = lax.all_to_all(summed, "dp", split_axis=0, concat_axis=2, tiled=True)
        wide = wide.reshape(rows // groups, -1)
        image_rows = lax.all_to_all(wide, "tensor", split_axis=1, concat_axis=0, tiled=True)
        return jnp.pad(image_rows, ((0, slots - rows), (0, 0)))

    buckets = (slots * 3 // 4, slots)
    image_rows = lax.cond(
        most <= buckets[0],
        lambda: image_part(buckets[0]),
        lambda: image_part(buckets[1]),
    )
    image_rows = (image_rows.astype(jnp.float32) + second_bias).astype(jnp.bfloat16)
    image_rows = jnp.pad(image_rows, ((0, seq_rows - slots), (0, 0)))
    row_ids = jnp.arange(seq_rows, dtype=jnp.int32)[:, None]
    embeddings = jnp.where(row_ids < own(filled), image_rows, text_embeds)
    embed_values = embeddings.astype(jnp.float32)
    square_total = lax.psum(jnp.sum(embed_values * embed_values, axis=-1), "tensor")
    scale_rows = lax.rsqrt(square_total / (feature_width * groups) + 1e-06)
    normed = (embed_values * scale_rows[:, None] * final_gain).astype(jnp.bfloat16)
    return (embeddings, normed)


def solution(mesh):
    placed = (
        P("dp", None),
        P(),
        P(),
        P(None, "tensor"),
        P("tensor"),
        P("tensor", "dp"),
        P("tensor"),
        P("dp", "tensor"),
        P("tensor"),
        P(),
        P(),
    )
    return jax.shard_map(
        per_device,
        mesh=mesh,
        in_specs=placed,
        out_specs=(P("dp", "tensor"), P("dp", "tensor")),
        check_vma=False,
    )
```

```python
import functools

import jax
import jax.numpy as jnp
from jax import lax
from jax.experimental import pallas as pl
from jax.experimental.pallas import tpu as pltpu
from jax.sharding import PartitionSpec as P

VMEM_LIMIT = 56 * 1024 * 1024


def hidden_kernel(per_token, patches_ref, gain_ref, bias_ref, weight_ref, first_bias_ref, index_ref, out_ref, rows_ref, total_ref):
    step = pl.program_id(0)
    tokens = out_ref.shape[0]

    @pl.when(step == 0)
    def _():
        gain = gain_ref[...]
        bias = bias_ref[...]

        def chunk(i, carry):
            span = pl.ds(pl.multiple_of(i * 128, 128), 128)
            values = patches_ref[span, :].astype(jnp.float32)
            centered = values - jnp.mean(values, axis=-1, keepdims=True)
            variance = jnp.mean(centered * centered, axis=-1, keepdims=True)
            normed = centered * lax.rsqrt(variance + 1e-06) * gain + bias
            for c in range(normed.shape[1] // 128):
                rows_ref[c, span, :] = normed[:, c * 128:(c + 1) * 128]
            return carry

        lax.fori_loop(0, patches_ref.shape[0] // 128, chunk, 0)
        total_ref[...] = jnp.zeros_like(total_ref)

    strips = [rows_ref[c, pl.ds(step, tokens, stride=per_token), :] for c in range(rows_ref.shape[0])]
    merged = jnp.concatenate(strips, axis=1).astype(jnp.bfloat16)
    total_ref[...] += jnp.dot(merged, weight_ref[...], preferred_element_type=jnp.float32)

    @pl.when(step == per_token - 1)
    def _():
        x = total_ref[...] + first_bias_ref[...]
        hidden = (0.5 * x * (1.0 + lax.erf(x * (0.5 ** 0.5)))).astype(jnp.bfloat16)
        columns = lax.broadcasted_iota(jnp.int32, (tokens, tokens), 1)
        pick = (columns == index_ref[...]).astype(jnp.bfloat16)
        out_ref[...] = jnp.dot(pick, hidden, preferred_element_type=jnp.float32).astype(jnp.bfloat16)


def compact_hidden(patches, norm_gain, norm_bias, first_weight, first_bias, index):
    width = patches.shape[1]
    per_token = first_weight.shape[0] // width
    tokens = patches.shape[0] // per_token
    out_width = first_weight.shape[1]
    whole = lambda shape: pl.BlockSpec(shape, lambda j: (0,) * len(shape))
    return pl.pallas_call(
        functools.partial(hidden_kernel, per_token),
        grid=(per_token,),
        in_specs=[
            whole(patches.shape),
            whole((1, width)),
            whole((1, width)),
            pl.BlockSpec((width, out_width), lambda j: (j, 0)),
            whole((1, out_width)),
            whole((tokens, 1)),
        ],
        out_specs=whole((tokens, out_width)),
        out_shape=jax.ShapeDtypeStruct((tokens, out_width), jnp.bfloat16),
        scratch_shapes=[
            pltpu.VMEM((width // 128, patches.shape[0], 128), jnp.float32),
            pltpu.VMEM((tokens, out_width), jnp.float32),
        ],
        compiler_params=pltpu.CompilerParams(vmem_limit_bytes=VMEM_LIMIT),
        cost_estimate=pl.CostEstimate(
            flops=2 * tokens * first_weight.size, bytes_accessed=2 * first_weight.size, transcendentals=0
        ),
        name="compact_hidden",
    )(patches, norm_gain[None], norm_bias[None], first_weight, first_bias[None], index[:, None])


def project_kernel(strides, *refs):
    index_ref, weight_ref, out_ref = refs[strides], refs[strides + 1], refs[strides + 2]
    rows = out_ref.shape[1]
    index = index_ref[0]
    columns = lax.broadcasted_iota(jnp.int32, (rows, rows), 1)
    total = None
    for k in range(strides):
        pick = (columns + k * rows == index).astype(jnp.bfloat16)
        term = jnp.dot(pick, refs[k][0], preferred_element_type=jnp.float32)
        total = term if total is None else total + term
    out_ref[0] = jnp.dot(total.astype(jnp.bfloat16), weight_ref[...], preferred_element_type=jnp.float32).astype(jnp.bfloat16)


def project(gathered, second_weight, index, strides):
    shards, rows, depth = gathered.shape
    width = second_weight.shape[1]
    source = lambda k: pl.BlockSpec((1, rows, depth), lambda e: ((e + shards - k) % shards, 0, 0))
    return pl.pallas_call(
        functools.partial(project_kernel, strides),
        grid=(shards,),
        in_specs=[source(k) for k in range(strides)]
        + [pl.BlockSpec((1, rows, 1), lambda e: (e, 0, 0)), pl.BlockSpec((depth, width), lambda e: (0, 0))],
        out_specs=pl.BlockSpec((1, rows, width), lambda e: (e, 0, 0)),
        out_shape=jax.ShapeDtypeStruct((shards, rows, width), jnp.bfloat16),
        compiler_params=pltpu.CompilerParams(vmem_limit_bytes=VMEM_LIMIT),
        cost_estimate=pl.CostEstimate(
            flops=2 * shards * rows * depth * width, bytes_accessed=4 * gathered.size, transcendentals=0
        ),
        name="project",
    )(*([gathered] * strides), index[:, :, None], second_weight)


def gather_kernel(own_ref, out_ref, line_send, line_recv, pair_send, pair_recv):
    shards = out_ref.shape[0]
    length = shards // 2
    me = lax.axis_index("dp")
    place, row = me // 2, me % 2
    other = me + 1 - 2 * row
    barrier = pltpu.get_barrier_semaphore()
    pl.semaphore_signal(barrier, inc=1, device_id={"dp": other})

    @pl.when(place > 0)
    def _():
        pl.semaphore_signal(barrier, inc=1, device_id={"dp": me - 2})

    @pl.when(place < length - 1)
    def _():
        pl.semaphore_signal(barrier, inc=1, device_id={"dp": me + 2})

    peers = 1 + (place > 0).astype(jnp.int32) + (place < length - 1).astype(jnp.int32)
    pl.semaphore_wait(barrier, peers)

    def line_copy(block, way, src):
        return pltpu.make_async_remote_copy(
            src_ref=src,
            dst_ref=out_ref.at[2 * block + row],
            send_sem=line_send.at[(way + 1) // 2, block],
            recv_sem=line_recv.at[block],
            device_id={"dp": me + 2 * way},
        )

    def pair_copy(block, src, side):
        return pltpu.make_async_remote_copy(
            src_ref=src,
            dst_ref=out_ref.at[2 * block + side],
            send_sem=pair_send.at[block],
            recv_sem=pair_recv.at[block],
            device_id={"dp": other},
        )

    for step in range(length):
        for way in (1, -1):
            block = place - way * step
            src = own_ref if step == 0 else out_ref.at[2 * block + row]

            @pl.when((block >= 0) & (block < length))
            def _(way=way, block=block, src=src, step=step):
                if step > 0:
                    line_copy(block, way, src).wait_recv()

                @pl.when((place + way >= 0) & (place + way < length))
                def _():
                    line_copy(block, way, src).start()

                if step > 0 or way == 1:
                    pair_copy(block, src, row).start()

    out_ref[me] = own_ref[...]

    def drain(block, carry):
        here = out_ref.at[2 * block + row]
        pair_copy(block, here, 1 - row).wait_recv()
        pair_copy(block, here, row).wait_send()

        @pl.when((block <= place) & (place < length - 1))
        def _():
            line_copy(block, 1, here).wait_send()

        @pl.when((block >= place) & (place > 0))
        def _():
            line_copy(block, -1, here).wait_send()

        return carry

    lax.fori_loop(0, length, drain, 0)


def gathered_rows(own, call_id):
    shards = lax.axis_size("dp")
    dma = pltpu.SemaphoreType.DMA
    return pl.pallas_call(
        gather_kernel,
        in_specs=[pl.BlockSpec(memory_space=pltpu.VMEM)],
        out_specs=pl.BlockSpec(memory_space=pltpu.VMEM),
        out_shape=jax.ShapeDtypeStruct((shards,) + own.shape, own.dtype),
        scratch_shapes=[dma((2, shards // 2)), dma((shards // 2,)), dma((shards // 2,)), dma((shards // 2,))],
        compiler_params=pltpu.CompilerParams(
            collective_id=call_id, has_side_effects=True, vmem_limit_bytes=VMEM_LIMIT
        ),
        name="gather_rows",
    )(own)


def scatter_kernel(
    part_ref, out_ref, pair_in, cross_out, cross_in, ready, wide,
    pair_send, pair_recv, cross_send, cross_recv, wide_send, wide_recv, out_send, out_recv,
):
    shards, groups = part_ref.shape[0], part_ref.shape[1]
    per_group = shards // groups
    me = lax.axis_index("dp")
    group = lax.axis_index("tensor")
    core, side = group % 2, group // 2
    mate = 2 * side + 1 - core
    across = group + 2 - 4 * side
    across_mate = mate + 2 - 4 * side
    f32 = jnp.float32

    barrier = pltpu.get_barrier_semaphore()
    for peer in (mate, across, across_mate):
        pl.semaphore_signal(barrier, inc=1, device_id={"tensor": peer})

    def greet(i, carry):
        pl.semaphore_signal(barrier, inc=1, device_id={"dp": (me + 1 + i) % shards})
        return carry

    lax.fori_loop(0, shards - 1, greet, 0)
    pl.semaphore_wait(barrier, shards + 2)

    def pair_copy(e, slot):
        return pltpu.make_async_remote_copy(
            src_ref=part_ref.at[e, mate if slot == 0 else across_mate],
            dst_ref=pair_in.at[e, slot],
            send_sem=pair_send.at[slot, e],
            recv_sem=pair_recv.at[slot, e],
            device_id={"tensor": mate},
        )

    def cross_copy(e):
        return pltpu.make_async_remote_copy(
            src_ref=cross_out.at[e],
            dst_ref=cross_in.at[e],
            send_sem=cross_send.at[e],
            recv_sem=cross_recv.at[e],
            device_id={"tensor": across},
        )

    def wide_copy(e, source):
        return pltpu.make_async_remote_copy(
            src_ref=ready.at[e],
            dst_ref=wide.at[source],
            send_sem=wide_send.at[e],
            recv_sem=wide_recv.at[source],
            device_id={"dp": e},
        )

    def out_copy(source, target, sender):
        return pltpu.make_async_remote_copy(
            src_ref=wide.at[source],
            dst_ref=out_ref.at[sender, source % per_group],
            send_sem=out_send.at[source],
            recv_sem=out_recv.at[sender, source % per_group],
            device_id={"tensor": target},
        )

    def start_pair(i, carry):
        e = (me + 1 + i) % shards
        for slot in (1, 0):
            pair_copy(e, slot).start()
        return carry

    lax.fori_loop(0, shards, start_pair, 0)

    def start_cross(i, carry):
        e = (me + 1 + i) % shards
        pair_copy(e, 1).wait_recv()
        cross_out[e] = (part_ref[e, across].astype(f32) + pair_in[e, 1].astype(f32)).astype(jnp.bfloat16)
        cross_copy(e).start()
        return carry

    lax.fori_loop(0, shards, start_cross, 0)

    def forward(source):
        target = source // per_group

        @pl.when(target == group)
        def _():
            out_ref[group, source % per_group] = wide[source]

        @pl.when(target != group)
        def _():
            out_copy(source, target, group).start()

    lag = 2

    def start_wide(i, carry):
        @pl.when(i < shards)
        def _():
            e = (me + 1 + i) % shards
            pair_copy(e, 0).wait_recv()
            cross_copy(e).wait_recv()
            total = part_ref[e, group].astype(f32) + pair_in[e, 0].astype(f32) + cross_in[e].astype(f32)

            @pl.when(i < shards - 1)
            def _():
                ready[e] = total.astype(jnp.bfloat16)
                wide_copy(e, me).start()

            @pl.when(i == shards - 1)
            def _():
                wide[me] = total.astype(jnp.bfloat16)
                forward(me)

        @pl.when((i >= lag) & (i < shards - 1 + lag))
        def _():
            source = (me + 2 * shards - 1 - (i - lag)) % shards
            wide_copy(source, source).wait_recv()
            forward(source)

        return carry

    lax.fori_loop(0, shards + lag - 1, start_wide, 0)

    def drain(i, carry):
        e = (me + 1 + i) % shards
        for slot in (1, 0):
            pair_copy(e, slot).wait_send()
        cross_copy(e).wait_send()

        @pl.when(i < shards - 1)
        def _():
            wide_copy(e, me).wait_send()

        @pl.when(e // per_group != group)
        def _():
            out_copy(e, e // per_group, group).wait_send()

        return carry

    lax.fori_loop(0, shards, drain, 0)
    for peer in (mate, across, across_mate):

        def receive(c, carry, peer=peer):
            out_copy(group * per_group + c, peer, peer).wait_recv()
            return carry

        lax.fori_loop(0, per_group, receive, 0)


def scattered_rows(pieces, call_id):
    shards, groups, rows, width = pieces.shape
    dma = pltpu.SemaphoreType.DMA
    block = pltpu.VMEM((shards, rows, width), jnp.bfloat16)
    out = pl.pallas_call(
        scatter_kernel,
        in_specs=[pl.BlockSpec(memory_space=pltpu.VMEM)],
        out_specs=pl.BlockSpec(memory_space=pltpu.VMEM),
        out_shape=jax.ShapeDtypeStruct((groups, shards // groups, rows, width), jnp.bfloat16),
        scratch_shapes=[
            pltpu.VMEM((shards, 2, rows, width), jnp.bfloat16), block, block, block, block,
            dma((2, shards)), dma((2, shards)), dma((shards,)), dma((shards,)),
            dma((shards,)), dma((shards,)), dma((shards,)), dma((groups, shards // groups)),
        ],
        compiler_params=pltpu.CompilerParams(
            collective_id=call_id, has_side_effects=True, vmem_limit_bytes=VMEM_LIMIT
        ),
        name="scatter_rows",
    )(pieces)
    return out.transpose(0, 2, 1, 3).reshape(groups * rows, -1)


def per_device(
    patches,
    norm_gain,
    norm_bias,
    first_weight,
    first_bias,
    second_weight,
    second_bias,
    text_embeds,
    final_gain,
    image_grids,
    routing,
):
    own_index = lax.axis_index("dp")
    shards = lax.axis_size("dp")
    groups = lax.axis_size("tensor")
    strides = image_grids.shape[1]
    slots = patches.shape[0] * patches.shape[1] // first_weight.shape[0]
    cap = slots // strides
    seq_rows, feature_width = text_embeds.shape
    slot_ids = jnp.arange(strides, dtype=jnp.int32)
    lower = (slot_ids[:, None] < slot_ids[None, :]).astype(jnp.int32)

    is_at = (routing[:, None, :] == slot_ids[None, :, None]).astype(jnp.int32)
    areas = image_grids[:, :, 0] * image_grids[:, :, 1]
    counts = jnp.sum(is_at * areas[:, None, :], axis=-1)
    chosen = jnp.sum(is_at * slot_ids, axis=-1)
    starts = jnp.sum(counts[:, :, None] * lower, axis=1)
    arriving = jnp.stack([jnp.roll(counts[:, k], k) for k in range(strides)], axis=1)
    source_starts = jnp.stack([jnp.roll(starts[:, k], k) for k in range(strides)], axis=1)
    laid_at = jnp.sum(arriving[:, :, None] * lower, axis=1)
    filled = jnp.sum(arriving, axis=1)
    most = jnp.maximum(jnp.max(jnp.sum(counts, axis=1)), jnp.max(filled))

    position = jnp.arange(slots, dtype=jnp.int32)
    own = lambda table: lax.dynamic_index_in_dim(table, own_index, 0, keepdims=False)
    inside = position[:, None] - own(starts)[None, :]
    live = (inside >= 0) & (inside < own(counts)[None, :])
    own_pick = jnp.sum(jnp.where(live, own(chosen)[None, :] * cap + inside + 1, 0), axis=1) - 1
    hidden = compact_hidden(patches, norm_gain, norm_bias, first_weight, first_bias, own_pick)

    def image_part(rows, call_id):
        inside = position[None, :rows, None] - laid_at[:, None, :]
        live = (inside >= 0) & (inside < arriving[:, None, :])
        index = jnp.sum(
            jnp.where(live, slot_ids * rows + source_starts[:, None, :] + inside + 1, 0), axis=2
        ) - 1
        gathered = gathered_rows(hidden[:rows], 2 * call_id)
        partial_value = project(gathered, second_weight, index, strides)
        pieces = partial_value.reshape(shards, groups, rows // groups, -1)
        image_rows = scattered_rows(pieces, 2 * call_id + 1)
        return jnp.pad(image_rows, ((0, slots - rows), (0, 0)))

    buckets = (slots * 3 // 4, slots)
    image_rows = lax.cond(
        most <= buckets[0],
        lambda: image_part(buckets[0], 0),
        lambda: image_part(buckets[1], 1),
    )
    image_rows = (image_rows.astype(jnp.float32) + second_bias).astype(jnp.bfloat16)
    image_rows = jnp.pad(image_rows, ((0, seq_rows - slots), (0, 0)))
    row_ids = jnp.arange(seq_rows, dtype=jnp.int32)[:, None]
    embeddings = jnp.where(row_ids < own(filled), image_rows, text_embeds)
    embed_values = embeddings.astype(jnp.float32)
    square_total = lax.psum(jnp.sum(embed_values * embed_values, axis=-1), "tensor")
    scale_rows = lax.rsqrt(square_total / (feature_width * groups) + 1e-06)
    normed = (embed_values * scale_rows[:, None] * final_gain).astype(jnp.bfloat16)
    return (embeddings, normed)


def solution(mesh):
    placed = (
        P("dp", None),
        P(),
        P(),
        P(None, "tensor"),
        P("tensor"),
        P("tensor", "dp"),
        P("tensor"),
        P("dp", "tensor"),
        P("tensor"),
        P(),
        P(),
    )
    return jax.shard_map(
        per_device,
        mesh=mesh,
        in_specs=placed,
        out_specs=(P("dp", "tensor"), P("dp", "tensor")),
        check_vma=False,
    )
```

```python
import functools

import jax
import jax.numpy as jnp
from jax import lax
from jax.experimental import pallas as pl
from jax.experimental.pallas import tpu as pltpu
from jax.sharding import PartitionSpec as P

VMEM_LIMIT = 56 * 1024 * 1024


def hidden_kernel(per_token, patches_ref, gain_ref, bias_ref, weight_ref, first_bias_ref, index_ref, out_ref, rows_ref, total_ref):
    step = pl.program_id(0)
    tokens = out_ref.shape[0]

    @pl.when(step == 0)
    def _():
        gain = gain_ref[...][None, :]
        bias = bias_ref[...][None, :]

        def chunk(i, carry):
            span = pl.ds(pl.multiple_of(i * 128, 128), 128)
            values = patches_ref[span, :].astype(jnp.float32)
            centered = values - jnp.mean(values, axis=-1, keepdims=True)
            variance = jnp.mean(centered * centered, axis=-1, keepdims=True)
            normed = centered * lax.rsqrt(variance + 1e-06) * gain + bias
            for c in range(normed.shape[1] // 128):
                rows_ref[c, span, :] = normed[:, c * 128:(c + 1) * 128]
            return carry

        lax.fori_loop(0, patches_ref.shape[0] // 128, chunk, 0)
        total_ref[...] = jnp.zeros_like(total_ref)

    strips = [rows_ref[c, pl.ds(step, tokens, stride=per_token), :] for c in range(rows_ref.shape[0])]
    merged = jnp.concatenate(strips, axis=1).astype(jnp.bfloat16)
    total_ref[...] += jnp.dot(merged, weight_ref[...], preferred_element_type=jnp.float32)

    @pl.when(step == per_token - 1)
    def _():
        x = total_ref[...] + first_bias_ref[...][None, :]
        hidden = (0.5 * x * (1.0 + lax.erf(x * (0.5 ** 0.5)))).astype(jnp.bfloat16)
        columns = lax.broadcasted_iota(jnp.int32, (tokens, tokens), 1)
        pick = (columns == index_ref[...]).astype(jnp.bfloat16)
        out_ref[...] = jnp.dot(pick, hidden, preferred_element_type=jnp.float32).astype(jnp.bfloat16)


def compact_hidden(patches, norm_gain, norm_bias, first_weight, first_bias, index):
    width = patches.shape[1]
    per_token = first_weight.shape[0] // width
    tokens = patches.shape[0] // per_token
    out_width = first_weight.shape[1]
    whole = lambda shape: pl.BlockSpec(shape, lambda j: (0,) * len(shape))
    return pl.pallas_call(
        functools.partial(hidden_kernel, per_token),
        grid=(per_token,),
        in_specs=[
            whole(patches.shape),
            whole((width,)),
            whole((width,)),
            pl.BlockSpec((width, out_width), lambda j: (j, 0)),
            whole((out_width,)),
            whole((tokens, 1)),
        ],
        out_specs=whole((tokens, out_width)),
        out_shape=jax.ShapeDtypeStruct((tokens, out_width), jnp.bfloat16),
        scratch_shapes=[
            pltpu.VMEM((width // 128, patches.shape[0], 128), jnp.float32),
            pltpu.VMEM((tokens, out_width), jnp.float32),
        ],
        compiler_params=pltpu.CompilerParams(vmem_limit_bytes=VMEM_LIMIT),
        cost_estimate=pl.CostEstimate(
            flops=2 * tokens * first_weight.size, bytes_accessed=2 * first_weight.size, transcendentals=0
        ),
        name="compact_hidden",
    )(patches, norm_gain, norm_bias, first_weight, first_bias, index[:, None])


def project_kernel(strides, *refs):
    index_ref, weight_ref, out_ref = refs[strides], refs[strides + 1], refs[strides + 2]
    rows = out_ref.shape[1]
    index = index_ref[0]
    columns = lax.broadcasted_iota(jnp.int32, (rows, rows), 1)
    total = None
    for k in range(strides):
        pick = (columns + k * rows == index).astype(jnp.bfloat16)
        term = jnp.dot(pick, refs[k][0], preferred_element_type=jnp.float32)
        total = term if total is None else total + term
    out_ref[0] = jnp.dot(total.astype(jnp.bfloat16), weight_ref[...], preferred_element_type=jnp.float32).astype(jnp.bfloat16)


def project(gathered, second_weight, index, strides):
    shards, rows, depth = gathered.shape
    width = second_weight.shape[1]
    source = lambda k: pl.BlockSpec((1, rows, depth), lambda e: ((e + shards - k) % shards, 0, 0))
    return pl.pallas_call(
        functools.partial(project_kernel, strides),
        grid=(shards,),
        in_specs=[source(k) for k in range(strides)]
        + [pl.BlockSpec((1, rows, 1), lambda e: (e, 0, 0)), pl.BlockSpec((depth, width), lambda e: (0, 0))],
        out_specs=pl.BlockSpec((1, rows, width), lambda e: (e, 0, 0)),
        out_shape=jax.ShapeDtypeStruct((shards, rows, width), jnp.bfloat16),
        compiler_params=pltpu.CompilerParams(vmem_limit_bytes=VMEM_LIMIT),
        cost_estimate=pl.CostEstimate(
            flops=2 * shards * rows * depth * width, bytes_accessed=4 * gathered.size, transcendentals=0
        ),
        name="project",
    )(*([gathered] * strides), index[:, :, None], second_weight)


def gather_kernel(own_ref, out_ref, line_send, line_recv, pair_send, pair_recv):
    shards = out_ref.shape[0]
    length = shards // 2
    me = lax.axis_index("dp")
    place, row = me // 2, me % 2
    other = me + 1 - 2 * row
    barrier = pltpu.get_barrier_semaphore()
    pl.semaphore_signal(barrier, inc=1, device_id={"dp": other})

    @pl.when(place > 0)
    def _():
        pl.semaphore_signal(barrier, inc=1, device_id={"dp": me - 2})

    @pl.when(place < length - 1)
    def _():
        pl.semaphore_signal(barrier, inc=1, device_id={"dp": me + 2})

    peers = 1 + (place > 0).astype(jnp.int32) + (place < length - 1).astype(jnp.int32)
    pl.semaphore_wait(barrier, peers)

    def line_copy(block, way, src):
        return pltpu.make_async_remote_copy(
            src_ref=src,
            dst_ref=out_ref.at[2 * block + row],
            send_sem=line_send.at[(way + 1) // 2, block],
            recv_sem=line_recv.at[block],
            device_id={"dp": me + 2 * way},
        )

    def pair_copy(block, src, side):
        return pltpu.make_async_remote_copy(
            src_ref=src,
            dst_ref=out_ref.at[2 * block + side],
            send_sem=pair_send.at[block],
            recv_sem=pair_recv.at[block],
            device_id={"dp": other},
        )

    for step in range(length):
        for way in (1, -1):
            block = place - way * step
            src = own_ref if step == 0 else out_ref.at[2 * block + row]

            @pl.when((block >= 0) & (block < length))
            def _(way=way, block=block, src=src, step=step):
                if step > 0:
                    line_copy(block, way, src).wait_recv()

                @pl.when((place + way >= 0) & (place + way < length))
                def _():
                    line_copy(block, way, src).start()

                if step > 0 or way == 1:
                    pair_copy(block, src, row).start()

    out_ref[me] = own_ref[...]

    def drain(block, carry):
        here = out_ref.at[2 * block + row]
        pair_copy(block, here, 1 - row).wait_recv()
        pair_copy(block, here, row).wait_send()

        @pl.when((block <= place) & (place < length - 1))
        def _():
            line_copy(block, 1, here).wait_send()

        @pl.when((block >= place) & (place > 0))
        def _():
            line_copy(block, -1, here).wait_send()

        return carry

    lax.fori_loop(0, length, drain, 0)


def gathered_rows(own, call_id):
    shards = lax.axis_size("dp")
    dma = pltpu.SemaphoreType.DMA
    return pl.pallas_call(
        gather_kernel,
        in_specs=[pl.BlockSpec(memory_space=pltpu.VMEM)],
        out_specs=pl.BlockSpec(memory_space=pltpu.VMEM),
        out_shape=jax.ShapeDtypeStruct((shards,) + own.shape, own.dtype),
        scratch_shapes=[dma((2, shards // 2)), dma((shards // 2,)), dma((shards // 2,)), dma((shards // 2,))],
        compiler_params=pltpu.CompilerParams(
            collective_id=call_id, has_side_effects=True, vmem_limit_bytes=VMEM_LIMIT
        ),
        name="gather_rows",
    )(own)


def scatter_kernel(
    part_ref, out_ref, pair_in, cross_out, cross_in, ready, wide,
    pair_send, pair_recv, cross_send, cross_recv, wide_send, wide_recv, out_send, out_recv,
):
    shards, groups = part_ref.shape[0], part_ref.shape[1]
    per_group = shards // groups
    me = lax.axis_index("dp")
    group = lax.axis_index("tensor")
    core, side = group % 2, group // 2
    mate = 2 * side + 1 - core
    across = group + 2 - 4 * side
    across_mate = mate + 2 - 4 * side
    f32 = jnp.float32

    barrier = pltpu.get_barrier_semaphore()
    for peer in (mate, across, across_mate):
        pl.semaphore_signal(barrier, inc=1, device_id={"tensor": peer})

    def greet(i, carry):
        pl.semaphore_signal(barrier, inc=1, device_id={"dp": (me + 1 + i) % shards})
        return carry

    lax.fori_loop(0, shards - 1, greet, 0)
    pl.semaphore_wait(barrier, shards + 2)

    def pair_copy(e, slot):
        return pltpu.make_async_remote_copy(
            src_ref=part_ref.at[e, mate if slot == 0 else across_mate],
            dst_ref=pair_in.at[e, slot],
            send_sem=pair_send.at[slot, e],
            recv_sem=pair_recv.at[slot, e],
            device_id={"tensor": mate},
        )

    def cross_copy(e):
        return pltpu.make_async_remote_copy(
            src_ref=cross_out.at[e],
            dst_ref=cross_in.at[e],
            send_sem=cross_send.at[e],
            recv_sem=cross_recv.at[e],
            device_id={"tensor": across},
        )

    def wide_copy(e, source):
        return pltpu.make_async_remote_copy(
            src_ref=ready.at[e],
            dst_ref=wide.at[source],
            send_sem=wide_send.at[e],
            recv_sem=wide_recv.at[source],
            device_id={"dp": e},
        )

    def out_copy(source, target, sender):
        return pltpu.make_async_remote_copy(
            src_ref=wide.at[source],
            dst_ref=out_ref.at[sender, source % per_group],
            send_sem=out_send.at[source],
            recv_sem=out_recv.at[sender, source % per_group],
            device_id={"tensor": target},
        )

    def start_pair(i, carry):
        e = (me + 1 + i) % shards
        for slot in (1, 0):
            pair_copy(e, slot).start()
        return carry

    lax.fori_loop(0, shards, start_pair, 0)

    def start_cross(i, carry):
        e = (me + 1 + i) % shards
        pair_copy(e, 1).wait_recv()
        cross_out[e] = (part_ref[e, across].astype(f32) + pair_in[e, 1].astype(f32)).astype(jnp.bfloat16)
        cross_copy(e).start()
        return carry

    lax.fori_loop(0, shards, start_cross, 0)

    def forward(source):
        target = source // per_group

        @pl.when(target == group)
        def _():
            out_ref[group, source % per_group] = wide[source]

        @pl.when(target != group)
        def _():
            out_copy(source, target, group).start()

    lag = 2

    def start_wide(i, carry):
        @pl.when(i < shards)
        def _():
            e = (me + 1 + i) % shards
            pair_copy(e, 0).wait_recv()
            cross_copy(e).wait_recv()
            total = part_ref[e, group].astype(f32) + pair_in[e, 0].astype(f32) + cross_in[e].astype(f32)

            @pl.when(i < shards - 1)
            def _():
                ready[e] = total.astype(jnp.bfloat16)
                wide_copy(e, me).start()

            @pl.when(i == shards - 1)
            def _():
                wide[me] = total.astype(jnp.bfloat16)
                forward(me)

        @pl.when((i >= lag) & (i < shards - 1 + lag))
        def _():
            source = (me + 2 * shards - 1 - (i - lag)) % shards
            wide_copy(source, source).wait_recv()
            forward(source)

        return carry

    lax.fori_loop(0, shards + lag - 1, start_wide, 0)

    def drain(i, carry):
        e = (me + 1 + i) % shards
        for slot in (1, 0):
            pair_copy(e, slot).wait_send()
        cross_copy(e).wait_send()

        @pl.when(i < shards - 1)
        def _():
            wide_copy(e, me).wait_send()

        @pl.when(e // per_group != group)
        def _():
            out_copy(e, e // per_group, group).wait_send()

        return carry

    lax.fori_loop(0, shards, drain, 0)
    for peer in (mate, across, across_mate):

        def receive(c, carry, peer=peer):
            out_copy(group * per_group + c, peer, peer).wait_recv()
            return carry

        lax.fori_loop(0, per_group, receive, 0)


def scattered_rows(pieces, call_id):
    shards, groups, rows, width = pieces.shape
    dma = pltpu.SemaphoreType.DMA
    block = pltpu.VMEM((shards, rows, width), jnp.bfloat16)
    out = pl.pallas_call(
        scatter_kernel,
        in_specs=[pl.BlockSpec(memory_space=pltpu.VMEM)],
        out_specs=pl.BlockSpec(memory_space=pltpu.VMEM),
        out_shape=jax.ShapeDtypeStruct((groups, shards // groups, rows, width), jnp.bfloat16),
        scratch_shapes=[
            pltpu.VMEM((shards, 2, rows, width), jnp.bfloat16), block, block, block, block,
            dma((2, shards)), dma((2, shards)), dma((shards,)), dma((shards,)),
            dma((shards,)), dma((shards,)), dma((shards,)), dma((groups, shards // groups)),
        ],
        compiler_params=pltpu.CompilerParams(
            collective_id=call_id, has_side_effects=True, vmem_limit_bytes=VMEM_LIMIT
        ),
        name="scatter_rows",
    )(pieces)
    return out.transpose(0, 2, 1, 3).reshape(groups * rows, -1)


def per_device(
    patches,
    norm_gain,
    norm_bias,
    first_weight,
    first_bias,
    second_weight,
    second_bias,
    text_embeds,
    final_gain,
    image_grids,
    routing,
):
    own_index = lax.axis_index("dp")
    shards = lax.axis_size("dp")
    groups = lax.axis_size("tensor")
    strides = image_grids.shape[1]
    slots = patches.shape[0] * patches.shape[1] // first_weight.shape[0]
    cap = slots // strides
    seq_rows, feature_width = text_embeds.shape
    slot_ids = jnp.arange(strides, dtype=jnp.int32)
    lower = (slot_ids[:, None] < slot_ids[None, :]).astype(jnp.int32)

    is_at = (routing[:, None, :] == slot_ids[None, :, None]).astype(jnp.int32)
    areas = image_grids[:, :, 0] * image_grids[:, :, 1]
    counts = jnp.sum(is_at * areas[:, None, :], axis=-1)
    chosen = jnp.sum(is_at * slot_ids, axis=-1)
    starts = jnp.sum(counts[:, :, None] * lower, axis=1)
    arriving = jnp.stack([jnp.roll(counts[:, k], k) for k in range(strides)], axis=1)
    source_starts = jnp.stack([jnp.roll(starts[:, k], k) for k in range(strides)], axis=1)
    laid_at = jnp.sum(arriving[:, :, None] * lower, axis=1)
    filled = jnp.sum(arriving, axis=1)
    most = jnp.maximum(jnp.max(jnp.sum(counts, axis=1)), jnp.max(filled))

    position = jnp.arange(slots, dtype=jnp.int32)
    own = lambda table: lax.dynamic_index_in_dim(table, own_index, 0, keepdims=False)
    inside = position[:, None] - own(starts)[None, :]
    live = (inside >= 0) & (inside < own(counts)[None, :])
    own_pick = jnp.sum(jnp.where(live, own(chosen)[None, :] * cap + inside + 1, 0), axis=1) - 1
    hidden = compact_hidden(patches, norm_gain, norm_bias, first_weight, first_bias, own_pick)

    def image_part(rows, call_id):
        inside = position[None, :rows, None] - laid_at[:, None, :]
        live = (inside >= 0) & (inside < arriving[:, None, :])
        index = jnp.sum(
            jnp.where(live, slot_ids * rows + source_starts[:, None, :] + inside + 1, 0), axis=2
        ) - 1
        gathered = gathered_rows(hidden[:rows], 2 * call_id)
        partial_value = project(gathered, second_weight, index, strides)
        pieces = partial_value.reshape(shards, groups, rows // groups, -1)
        image_rows = scattered_rows(pieces, 2 * call_id + 1)
        return jnp.pad(image_rows, ((0, slots - rows), (0, 0)))

    buckets = (slots * 3 // 4, slots)
    image_rows = lax.cond(
        most <= buckets[0],
        lambda: image_part(buckets[0], 0),
        lambda: image_part(buckets[1], 1),
    )
    image_rows = (image_rows.astype(jnp.float32) + second_bias).astype(jnp.bfloat16)
    image_rows = jnp.pad(image_rows, ((0, seq_rows - slots), (0, 0)))
    row_ids = jnp.arange(seq_rows, dtype=jnp.int32)[:, None]
    embeddings = jnp.where(row_ids < own(filled), image_rows, text_embeds)
    embed_values = embeddings.astype(jnp.float32)
    square_total = lax.psum(jnp.sum(embed_values * embed_values, axis=-1), "tensor")
    scale_rows = lax.rsqrt(square_total / (feature_width * groups) + 1e-06)
    normed = (embed_values * scale_rows[:, None] * final_gain).astype(jnp.bfloat16)
    return (embeddings, normed)


def solution(mesh):
    placed = (
        P("dp", None),
        P(),
        P(),
        P(None, "tensor"),
        P("tensor"),
        P("tensor", "dp"),
        P("tensor"),
        P("dp", "tensor"),
        P("tensor"),
        P(),
        P(),
    )
    return jax.shard_map(
        per_device,
        mesh=mesh,
        in_specs=placed,
        out_specs=(P("dp", "tensor"), P("dp", "tensor")),
        check_vma=False,
    )
```
